32 devices in a mesh: group: 2 (over x), dp: 4 (over y, core), tensor: 4 (over z).
Axes of the slice: x: 2, y: 2, z: 4, core: 2. Of those that a mesh axis runs over, the one named last changes fastest.
Arguments:
- tokens: bfloat16 [1024, 5120], P(('group', 'dp'), 'tensor'), parts along dimension 0, may hold values from -6 to 6
- router: bfloat16 [5120, 2], replicated, may hold values from -0.078125 to 0.078125
- expert_gate: bfloat16 [5120, 8192], P(None, ('dp', 'tensor')), may hold values from -0.078125 to 0.078125
- expert_up: bfloat16 [5120, 8192], P(None, ('dp', 'tensor')), may hold values from -0.078125 to 0.078125
- expert_down: bfloat16 [8192, 5120], P(('dp', 'tensor')), may hold values from -0.09375 to 0.09375
- shared_gate: bfloat16 [5120, 4096], P('dp', 'tensor'), may hold values from -0.078125 to 0.078125
- shared_up: bfloat16 [5120, 4096], P('dp', 'tensor'), may hold values from -0.078125 to 0.078125
- shared_down: bfloat16 [4096, 5120], P('tensor', 'dp'), may hold values from -0.09375 to 0.09375
- expert_ids: int32 [1024], P(('group', 'dp')), parts along dimension 0, may hold values from 0 to 1, as said below
- expert_slots: int32 [1024], P(('group', 'dp')), parts along dimension 0, may hold values from 0 to 63, as said below
Outputs:
- mixed: bfloat16 [1024, 5120], P(('group', 'dp'), 'tensor'), parts along dimension 0
The draws below stay inside these ranges and needn't reach their ends.
There are 2 independent parts, one for each index of `group`. The reference program is written for one: setup_inputs(seed, part) draws one part's arguments, and reference() takes and returns one part's arrays. A program takes and returns all parts, laid end to end along the dimension named above; an argument that names none is the same for every part. Nothing has to cross between parts.
Inputs may be any that keep to these rules, and one draw needn't show every extreme that they name: `expert_ids`: among the tokens of one index of dp no expert has more than 64; in every draw one expert has exactly 64 tokens from every index of dp. `expert_slots`: tokens of one index of dp with the same expert have distinct slots.
All inputs are finite; a program needn't handle non-finite values.
Results may differ from the reference program's by a relative error of at most 0.015.
Values may be sent and summed in bfloat16 or wider, within the bound.
A program may use at most 128 MiB of HBM per device.

```python
import jax
import jax.numpy as jnp
from jax import lax

D = 5120
FFE = 4096
FFS = 4096
TOK_DEV = 128
EXPERTS = 2
CAP = 64
TOKENS = 512
N_DP = 4
N_TENSOR = 4


def routing_pairs(key):
    base = jax.random.fold_in(key, 101)
    busiest = jax.random.randint(jax.random.fold_in(base, 1), (), 0, EXPERTS)
    block_count = TOKENS // TOK_DEV
    pair_count = EXPERTS * CAP

    def one_block(block_key):
        rank_key, jitter_key, placing_key = jax.random.split(block_key, 3)
        pair_index = jnp.arange(pair_count, dtype=jnp.int32)
        expert = pair_index // CAP
        ranking = jax.random.permutation(rank_key, EXPERTS).astype(jnp.int32)
        jitter = jax.random.randint(jitter_key, (pair_count,), 0, 4096)
        scores = jitter + ranking[expert] * 512 + jnp.where(expert == busiest, 65536, 0)
        scores = scores * pair_count + pair_index
        chosen = lax.top_k(scores, TOK_DEV)[1].astype(jnp.int32)
        placing = jax.random.permutation(placing_key, TOK_DEV)
        expert_of = jnp.zeros((TOK_DEV,), jnp.int32).at[placing].set(chosen // CAP)
        slot_of = jnp.zeros((TOK_DEV,), jnp.int32).at[placing].set(chosen % CAP)
        return (expert_of, slot_of)
    block_keys = jax.random.split(jax.random.fold_in(base, 2), block_count)
    expert_of, slot_of = jax.vmap(one_block)(block_keys)
    return (expert_of.reshape(TOKENS), slot_of.reshape(TOKENS))


def draw_expert_ids(key, part):
    return routing_pairs(key)[0]


def draw_expert_slots(key, part):
    return routing_pairs(key)[1]


def levels(rng, extent, shards, low, high):
    def one(axis_at, parts):
        draws = jax.random.uniform(jax.random.fold_in(jax.random.fold_in(rng, 6), axis_at), (parts,), jnp.float32, low / len(shards), high / len(shards))
        return jnp.repeat(jnp.exp(draws), extent[axis_at] // parts).reshape((-1,) + (1,) * (len(extent) - axis_at - 1))

    factor_of = one(*shards[0])
    for cut in shards[1:]:
        factor_of = factor_of * one(*cut)
    return factor_of


def gaussian(rng, dims, deviation, limit, cuts=(), held_as=jnp.bfloat16):
    result = jax.random.normal(rng, dims, jnp.float32) * deviation
    if len(cuts) > 0:
        result = levels(rng, dims, cuts, -0.22, 0.18) * result
    return jnp.clip(result, min=-limit, max=limit).astype(held_as)


def setup_inputs(seed: int = 0, part: int = 0) -> dict:
    splits = jax.random.split(jax.random.key(seed), 11)
    part_splits = jax.random.split(jax.random.fold_in(splits[10], part), 11)
    return {
        "tokens": gaussian(part_splits[0], (TOKENS, D), 1.0, 6.0, ((0, 4), (1, 4))),
        "router": gaussian(splits[1], (D, EXPERTS), D ** -0.5, 0.078125),
        "expert_gate": gaussian(splits[2], (D, EXPERTS * FFE), D ** -0.5, 0.078125, ((1, 16),)),
        "expert_up": gaussian(splits[3], (D, EXPERTS * FFE), D ** -0.5, 0.078125, ((1, 16),)),
        "expert_down": gaussian(splits[4], (EXPERTS * FFE, D), FFE ** -0.5, 0.09375, ((0, 16),)),
        "shared_gate": gaussian(splits[5], (D, FFS), D ** -0.5, 0.078125, ((0, 4), (1, 4))),
        "shared_up": gaussian(splits[6], (D, FFS), D ** -0.5, 0.078125, ((0, 4), (1, 4))),
        "shared_down": gaussian(splits[7], (FFS, D), FFS ** -0.5, 0.09375, ((0, 4), (1, 4))),
        "expert_ids": draw_expert_ids(jax.random.fold_in(jax.random.fold_in(splits[10], part), 71), part),
        "expert_slots": draw_expert_slots(jax.random.fold_in(jax.random.fold_in(splits[10], part), 71), part),
    }


def rounded_blocks(hidden, weight, block_count):
    row_count = hidden.shape[0]
    block_width = hidden.shape[1] // block_count
    hidden_blocks = hidden.reshape(row_count, block_count, block_width).transpose(1, 0, 2)
    weight_blocks = weight.reshape(block_count, block_width, weight.shape[1])

    def accumulate(running, inputs):
        portion = jnp.dot(inputs[0], inputs[1], preferred_element_type=jnp.float32).astype(jnp.bfloat16)
        portion = lax.optimization_barrier(portion)
        return running + portion.astype(jnp.float32), None

    running, _ = lax.scan(accumulate, jnp.zeros((row_count, weight.shape[1]), jnp.float32), (hidden_blocks, weight_blocks))
    return running


def reference(tokens, router, expert_gate, expert_up, expert_down, shared_gate, shared_up, shared_down, expert_ids, expert_slots):
    logits = jnp.dot(tokens, router, preferred_element_type=jnp.float32)
    one_hot = (expert_ids[:, None] == jnp.arange(EXPERTS, dtype=jnp.int32)[None, :]).astype(jnp.float32)
    gating = jax.nn.sigmoid(jnp.sum(logits * one_hot, axis=1))
    routed = (tokens.astype(jnp.float32) * gating[:, None]).astype(jnp.bfloat16)
    source_index = (jnp.arange(TOKENS, dtype=jnp.int32) // TOK_DEV).astype(jnp.int32)
    slot_row = (source_index * CAP + expert_slots).astype(jnp.int32)
    slot_table = jnp.zeros((EXPERTS, N_DP * CAP, D), jnp.bfloat16).at[expert_ids, slot_row].set(routed)
    gate_stack = expert_gate.reshape(D, EXPERTS, FFE).transpose(1, 0, 2)
    up_stack = expert_up.reshape(D, EXPERTS, FFE).transpose(1, 0, 2)
    down_stack = expert_down.reshape(EXPERTS, FFE, D)

    def one_expert(inputs):
        table, gate_w, up_w, down_w = inputs
        gate_sum = jnp.dot(table, gate_w, preferred_element_type=jnp.float32)
        up_sum = jnp.dot(table, up_w, preferred_element_type=jnp.float32)
        expert_hidden = (jax.nn.silu(gate_sum) * up_sum).astype(jnp.bfloat16)
        return rounded_blocks(expert_hidden, down_w, 2 * N_TENSOR).astype(jnp.bfloat16)

    expert_table = lax.map(one_expert, (slot_table, gate_stack, up_stack, down_stack))
    expert_out = expert_table[expert_ids, slot_row]
    shared_gate_sum = jnp.dot(tokens, shared_gate, preferred_element_type=jnp.float32)
    shared_up_sum = jnp.dot(tokens, shared_up, preferred_element_type=jnp.float32)
    shared_hidden = (jax.nn.silu(shared_gate_sum) * shared_up_sum).astype(jnp.bfloat16)
    shared_out = rounded_blocks(shared_hidden, shared_down, N_TENSOR)
    return (shared_out + expert_out.astype(jnp.float32)).astype(jnp.bfloat16)
```

```python
import functools

import jax
import jax.numpy as jnp
from jax import lax
from jax.experimental import pallas as pl
from jax.experimental.pallas import tpu as pltpu
from jax.sharding import PartitionSpec as P


def on_device(
    tokens,
    router,
    expert_gate,
    expert_up,
    expert_down,
    shared_gate,
    shared_up,
    shared_down,
    expert_ids,
    expert_slots,
):
    tok_rows, part_width = tokens.shape
    dp_count = lax.axis_size("dp")
    experts = dp_count // 2
    capacity = min(2 * tok_rows // experts, tok_rows // 2)
    gathered = lax.all_gather(tokens, "tensor", axis=1, tiled=True)
    logits = jnp.dot(gathered, router, preferred_element_type=jnp.float32)
    one_hot = (expert_ids[:, None] == jnp.arange(experts, dtype=jnp.int32)[None, :]).astype(
        jnp.float32
    )
    gating = jax.nn.sigmoid(jnp.sum(logits * one_hot, axis=1))
    routed = (tokens.astype(jnp.float32) * gating[:, None]).astype(jnp.bfloat16)
    outgoing = (
        jnp.zeros((experts, capacity, part_width), jnp.bfloat16)
        .at[expert_ids, expert_slots]
        .set(routed)
    )
    gate_sum = jnp.dot(
        gathered,
        lax.all_gather(shared_gate, "dp", axis=0, tiled=True),
        preferred_element_type=jnp.float32,
    )
    up_sum = jnp.dot(
        gathered,
        lax.all_gather(shared_up, "dp", axis=0, tiled=True),
        preferred_element_type=jnp.float32,
    )
    shared_hidden = (jax.nn.silu(gate_sum) * up_sum).astype(jnp.bfloat16)
    shared_terms = jnp.dot(
        shared_hidden,
        lax.all_gather(shared_down, "dp", axis=1, tiled=True),
        preferred_element_type=jnp.float32,
    )
    shared_out = lax.psum_scatter(
        shared_terms.astype(jnp.bfloat16), "tensor", scatter_dimension=1, tiled=True
    ).astype(jnp.float32)
    to_send = jnp.repeat(outgoing, 2, axis=0)
    received = lax.all_to_all(to_send, "dp", split_axis=0, concat_axis=0, tiled=True)
    source_count = received.shape[0]
    slot_count = received.shape[1]
    slot_total = source_count * slot_count
    portion = lax.all_gather(received, "tensor", axis=2, tiled=True)
    flattened = portion.reshape(slot_total, portion.shape[2])
    gate_e = jnp.dot(flattened, expert_gate, preferred_element_type=jnp.float32)
    up_e = jnp.dot(flattened, expert_up, preferred_element_type=jnp.float32)
    hidden_e = (jax.nn.silu(gate_e) * up_e).astype(jnp.bfloat16)
    expert_terms = jnp.dot(hidden_e, expert_down, preferred_element_type=jnp.float32)
    expert_terms = expert_terms.reshape(source_count, slot_count, expert_terms.shape[1])
    returned_raw = lax.all_to_all(
        lax.psum_scatter(
            expert_terms.astype(jnp.bfloat16), "tensor", scatter_dimension=2, tiled=True
        ),
        "dp",
        split_axis=0,
        concat_axis=0,
        tiled=True,
    ).astype(jnp.float32)
    returned = (
        returned_raw.reshape(experts, 2, capacity, part_width).sum(axis=1).astype(jnp.bfloat16)
    )
    expert_out = returned[expert_ids, expert_slots]
    return (shared_out + expert_out.astype(jnp.float32)).astype(jnp.bfloat16)


VMEM_BYTES = 64 * 1024 * 1024 - 65536


def tile_of(width):
    return next(t for t in (256, 128, width) if width % t == 0)


def layer_kernel(
    shape,
    tok, pick, unpick, router,
    eg_hbm, eu_hbm, ed_hbm, sg_hbm, su_hbm, sd_hbm,
    out,
    eg, eu, ed, sg, su, sd,
    own, table, rest, logit, acc_g, acc_u, hid_e, part_e, core_e, row_e, pair_e,
    part_s, got_s, hid_s, down_s, gotd_s, left, right, passed,
    wsem, send_y, recv_y, send_q, recv_q, send_ql, send_qr, send_l, send_r, recv_z, send_c, recv_c,
    send_pc, recv_pc, send_py, recv_py, send_gs, recv_gs, send_h, recv_h, send_d, recv_d,
    send_tr, send_tl, recv_tl, recv_tr,
):
    ndp, nt, cap, width = shape
    group, dp, z = (lax.axis_index(n) for n in ("group", "dp", "tensor"))
    y, c = lax.div(dp, 2), lax.rem(dp, 2)
    mate, across = 2 * y + 1 - c, 2 * (1 - y) + c
    others = [lax.rem(dp + i, ndp) for i in range(1, ndp)]
    rows = ndp * cap
    sending = []

    def copy(src, dst, ss, rs, dev_dp, dev_z):
        return pltpu.make_async_remote_copy(
            src_ref=src, dst_ref=dst, send_sem=ss, recv_sem=rs,
            device_id=(group, dev_dp, dev_z), device_id_type=pl.DeviceIdType.MESH,
        )

    def send(cond, make):
        if cond is None:
            make().start()
        else:
            pl.when(cond)(lambda: make().start())
        sending.append((cond, make))

    weights = [
        pltpu.make_async_copy(a, b, wsem.at[i])
        for i, (a, b) in enumerate(
            ((sg_hbm, sg), (su_hbm, su), (eg_hbm, eg), (eu_hbm, eu), (ed_hbm, ed), (sd_hbm, sd))
        )
    ]
    for w in weights:
        w.start()

    barrier = pltpu.get_barrier_semaphore()
    for o in others:
        pl.semaphore_signal(barrier, 1, device_id=(group, o, z), device_id_type=pl.DeviceIdType.MESH)

    @pl.when(z > 0)
    def _():
        pl.semaphore_signal(barrier, 1, device_id=(group, dp, z - 1), device_id_type=pl.DeviceIdType.MESH)

    @pl.when(z < nt - 1)
    def _():
        pl.semaphore_signal(barrier, 1, device_id=(group, dp, z + 1), device_id_type=pl.DeviceIdType.MESH)

    tw = tile_of(width)

    @pl.loop(0, width // tw)
    def _(i):
        cols = pl.ds(pl.multiple_of(i * tw, tw), tw)
        picked = jnp.dot(pick[...], tok[:, cols], preferred_element_type=jnp.float32)
        own[:, :, cols] = picked.astype(jnp.bfloat16).reshape(2, cap, tw)

    table[z, dp] = own[y]

    @pl.when(dp == z)
    def _():
        rest[dp] = own[1 - y]

    at_end = (z == 0) | (z == nt - 1)

    @pl.when(at_end)
    def _():
        pl.semaphore_wait(barrier, ndp)

    @pl.when(jnp.logical_not(at_end))
    def _():
        pl.semaphore_wait(barrier, ndp + 1)

    send(None, lambda: copy(own.at[1 - y], table.at[z, dp], send_y, recv_y, across, z))
    home_row = lax.div(z, 2)
    send(dp != z, lambda: copy(own.at[1 - home_row], rest.at[dp], send_q, recv_q.at[dp], z, z))

    def spread(zs, j, toward_left, toward_right):
        block = table.at[zs, 2 * j + c]
        send(toward_right, lambda: copy(block, block, send_r.at[zs, j], recv_z.at[zs, j], dp, z + 1))
        send(toward_left, lambda: copy(block, block, send_l.at[zs, j], recv_z.at[zs, j], dp, z - 1))

    def to_mate(cond, zs, j):
        block = table.at[zs, 2 * j + c]
        send(cond, lambda: copy(block, block, send_c.at[zs, j], recv_c.at[zs, j], mate, z))

    spread(z, y, z > 0, z < nt - 1)
    to_mate(None, z, y)
    copy(own.at[0], table.at[z, across], send_y, recv_y, across, z).wait_recv()
    spread(z, 1 - y, z > 0, z < nt - 1)
    to_mate(None, z, 1 - y)

    def relay_rest(distance):
        for s in range(ndp):
            for at, go_left, go_right in (
                ((z == dp, z > 0, z < nt - 1),)
                if distance == 0
                else (
                    (z == dp + distance, None, z < nt - 1),
                    (z == dp - distance, z > 0, None),
                )
            ):
                waits = at & (dp != s) if distance == 0 else at

                @pl.when(waits)
                def _():
                    copy(rest.at[s], rest.at[s], send_q, recv_q.at[s], dp, z).wait_recv()

                if go_left is not None:
                    send(at & go_left, lambda s=s: copy(
                        rest.at[s], rest.at[s], send_ql.at[s], recv_q.at[s], dp, z - 1))
                if go_right is not None:
                    send(at & go_right, lambda s=s: copy(
                        rest.at[s], rest.at[s], send_qr.at[s], recv_q.at[s], dp, z + 1))

    te = tile_of(acc_g.shape[1])

    logit[...] = jnp.zeros_like(logit)
    acc_g[...] = jnp.zeros_like(acc_g)
    acc_u[...] = jnp.zeros_like(acc_u)

    def expert_chunk(zs):
        for j in range(2):
            block = table.at[zs, 2 * j + 1 - c]
            copy(block, block, send_c.at[zs, j], recv_c.at[zs, j], mate, z).wait_recv()
        depth = pl.ds(pl.multiple_of(zs * width, width), width)
        x = table.at[zs]
        logit[...] += jnp.dot(
            x[...].reshape(rows, width), router[depth, :], preferred_element_type=jnp.float32
        )

        @pl.loop(0, acc_g.shape[1] // te)
        def _(i):
            cols = pl.ds(pl.multiple_of(i * te, te), te)
            xs = x[...].reshape(rows, width)
            acc_g[:, cols] += jnp.dot(xs, eg[depth, cols], preferred_element_type=jnp.float32)
            acc_u[:, cols] += jnp.dot(xs, eu[depth, cols], preferred_element_type=jnp.float32)

    relay_rest(0)
    for distance in range(1, nt):
        for zs, inside, far in (
            (z - distance, z >= distance, "right"),
            (z + distance, z + distance < nt, "left"),
        ):
            for jr in range(2):
                j = y if jr == 0 else 1 - y

                @pl.when(inside)
                def _():
                    block = table.at[zs, 2 * j + c]
                    copy(block, block, send_r.at[zs, j], recv_z.at[zs, j], dp, z).wait_recv()

                block = lambda zs=zs, j=j: table.at[zs, 2 * j + c]
                if far == "right":
                    send(inside & (z < nt - 1), lambda zs=zs, j=j, block=block: copy(
                        block(), block(), send_r.at[zs, j], recv_z.at[zs, j], dp, z + 1))
                else:
                    send(inside & (z > 0), lambda zs=zs, j=j, block=block: copy(
                        block(), block(), send_l.at[zs, j], recv_z.at[zs, j], dp, z - 1))
                send(inside, lambda zs=zs, j=j, block=block: copy(
                    block(), block(), send_c.at[zs, j], recv_c.at[zs, j], mate, z))
        relay_rest(distance)
        if distance == 1:
            for w in weights[:4]:
                w.wait()
            expert_chunk(z)
        else:
            for zs, inside in ((z - distance + 1, z >= distance - 1), (z + distance - 1, z + distance - 1 < nt)):
                pl.when(inside)(functools.partial(expert_chunk, zs))
    last = nt - 1
    for zs, inside in ((z - last, z >= last), (z + last, z + last < nt)):
        pl.when(inside)(functools.partial(expert_chunk, zs))

    hs = sg.shape[1]
    ts = tile_of(hs)

    @pl.loop(0, hs // ts)
    def _(i):
        cols = pl.ds(pl.multiple_of(i * ts, ts), ts)
        for w, k in ((sg, 0), (su, 1)):
            for src, e in ((table.at[dp], y), (rest, 1 - y)):
                part = jnp.dot(
                    src[...].reshape(rows, width), w[:, cols], preferred_element_type=jnp.float32
                )
                part_s[:, k, e, :, cols] = part.astype(jnp.bfloat16).reshape(ndp, cap, ts)

    for i, o in enumerate(others):
        send(None, lambda i=i, o=o: copy(
            part_s.at[o], got_s.at[i], send_gs.at[i], recv_gs.at[i], o, z))

    lanes = lax.broadcasted_iota(jnp.int32, logit.shape, 1)
    gating = jax.nn.sigmoid(jnp.sum(jnp.where(lanes == y, logit[...], 0.0), axis=1, keepdims=True))
    hid_e[...] = (jax.nn.silu(acc_g[...] * gating) * (acc_u[...] * gating)).astype(jnp.bfloat16)
    weights[4].wait()
    per = width // tw

    @pl.loop(0, nt * per)
    def _(i):
        t, n = lax.div(i, per), lax.rem(i, per)
        part = jnp.dot(
            hid_e[...], ed[:, pl.ds(pl.multiple_of(i * tw, tw), tw)],
            preferred_element_type=jnp.float32,
        )
        part_e[:, t, :, pl.ds(pl.multiple_of(n * tw, tw), tw)] = part.astype(
            jnp.bfloat16
        ).reshape(ndp, cap, tw)

    for j in range(2):
        send(None, lambda j=j: copy(
            part_e.at[2 * j + 1 - c], core_e.at[j], send_pc.at[j], recv_pc.at[j], mate, z))

    for i in range(ndp - 1):
        copy(part_s.at[0], got_s.at[i], send_gs.at[i], recv_gs.at[i], dp, z).wait_recv()

    @pl.loop(0, hs // ts)
    def _(i):
        cols = pl.ds(pl.multiple_of(i * ts, ts), ts)
        total = part_s[dp, :, :, :, cols].astype(jnp.float32)
        for k in range(ndp - 1):
            total = total + got_s[k, :, :, :, cols].astype(jnp.float32)
        hid_s[dp, :, cols] = (jax.nn.silu(total[0]) * total[1]).astype(jnp.bfloat16).reshape(
            2 * cap, ts
        )

    for i, o in enumerate(others):
        send(None, lambda i=i, o=o: copy(
            hid_s.at[dp], hid_s.at[dp], send_h.at[i], recv_h.at[dp], o, z))

    for j in range(2):
        copy(part_e.at[0], core_e.at[j], send_pc.at[j], recv_pc.at[j], dp, z).wait_recv()

    @pl.loop(0, nt)
    def _(t):
        both = part_e[across, t].astype(jnp.float32) + core_e[1 - y, t].astype(jnp.float32)
        pair_e[t] = both.astype(jnp.bfloat16)

    send(None, lambda: copy(pair_e, row_e, send_py, recv_py, across, z))

    for o in others:
        copy(hid_s.at[o], hid_s.at[o], send_h.at[0], recv_h.at[o], dp, z).wait_recv()
    weights[5].wait()

    @pl.loop(0, width // tw)
    def _(i):
        cols = pl.ds(pl.multiple_of(i * tw, tw), tw)
        part = jnp.dot(
            hid_s[...].reshape(ndp * 2 * cap, hs), sd[:, cols], preferred_element_type=jnp.float32
        )
        down_s[:, :, :, cols] = part.astype(jnp.bfloat16).reshape(ndp, 2, cap, tw)

    for i, o in enumerate(others):
        send(None, lambda i=i, o=o: copy(
            down_s.at[o], gotd_s.at[dp], send_d.at[i], recv_d.at[dp], o, z))
    gotd_s[dp] = down_s[dp]
    for o in others:
        copy(gotd_s.at[o], gotd_s.at[o], send_d.at[0], recv_d.at[o], dp, z).wait_recv()
    copy(pair_e, row_e, send_py, recv_py, dp, z).wait_recv()

    def own_sum(t, e, cols):
        shared = gotd_s[t, e, :, cols].astype(jnp.float32)
        near = part_e[dp, t, :, cols].astype(jnp.float32) + core_e[y, t, :, cols].astype(jnp.float32)
        return shared + jnp.where(e == y, near, row_e[t, :, cols].astype(jnp.float32))

    def combined(t, target, sources):
        @pl.loop(0, per)
        def _(i):
            cols = pl.ds(pl.multiple_of(i * tw, tw), tw)
            for e in range(2):
                total = own_sum(t, e, cols)
                for cond, ref in sources:
                    total = total + jnp.where(cond, ref[t, e, :, cols].astype(jnp.float32), 0.0)
                target[t, e, :, cols] = total.astype(jnp.bfloat16)

    def arrive(ref, sems, t, cond):
        @pl.when(cond)
        def _():
            copy(ref.at[t], ref.at[t], send_tr.at[t], sems.at[t], dp, z).wait_recv()

        @pl.when(jnp.logical_not(cond))
        def _():
            ref[t] = jnp.zeros(ref.shape[1:], ref.dtype)

    true = z >= 0
    for i in range(nt - 1):
        t = nt - 1 - i

        @pl.when(t > z)
        def _():
            arrive(left, recv_tl, t, z > 0)
            combined(t, passed, ((true, left),))

        send(t > z, lambda t=t: copy(
            passed.at[t], left.at[t], send_tr.at[t], recv_tl.at[t], dp, z + 1))
        u = i

        @pl.when(u < z)
        def _():
            arrive(right, recv_tr, u, z < nt - 1)
            combined(u, passed, ((true, right),))

        send(u < z, lambda u=u: copy(
            passed.at[u], right.at[u], send_tl.at[u], recv_tr.at[u], dp, z - 1))
    arrive(left, recv_tl, z, z > 0)
    arrive(right, recv_tr, z, z < nt - 1)
    combined(z, passed, ((true, left), (true, right)))

    @pl.loop(0, per)
    def _(i):
        cols = pl.ds(pl.multiple_of(i * tw, tw), tw)
        slots = passed[z, :, :, cols].reshape(2 * cap, tw)
        out[:, cols] = jnp.dot(unpick[...], slots, preferred_element_type=jnp.float32).astype(
            jnp.bfloat16
        )

    for cond, make in sending:
        if cond is None:
            make().wait_send()
        else:
            pl.when(cond)(lambda make=make: make().wait_send())


def fused(tokens, router, eg, eu, ed, sg, su, sd, ids, slots):
    ndp, nt = lax.axis_size("dp"), lax.axis_size("tensor")
    tok_rows, width = tokens.shape
    cap = min(2 * tok_rows // 2, tok_rows // 2)
    spot = ids * cap + slots
    pick = (jnp.arange(2 * cap, dtype=jnp.int32)[:, None] == spot[None, :]).astype(jnp.bfloat16)
    unpick = (spot[:, None] == jnp.arange(2 * cap, dtype=jnp.int32)[None, :]).astype(jnp.bfloat16)
    bf, f32 = jnp.bfloat16, jnp.float32
    rows, hid, hs, depth = ndp * cap, eg.shape[1], sg.shape[1], eg.shape[0]
    v = pltpu.VMEM
    dma = pltpu.SemaphoreType.DMA
    scratch = [v(w.shape, bf) for w in (eg, eu, ed, sg, su, sd)] + [
        v((2, cap, width), bf),
        v((nt, ndp, cap, width), bf),
        v((ndp, cap, width), bf),
        v((rows, router.shape[1]), f32),
        v((rows, hid), f32),
        v((rows, hid), f32),
        v((rows, hid), bf),
        v((ndp, nt, cap, width), bf),
        v((2, nt, cap, width), bf),
        v((nt, cap, width), bf),
        v((nt, cap, width), bf),
        v((ndp, 2, 2, cap, hs), bf),
        v((ndp - 1, 2, 2, cap, hs), bf),
        v((ndp, 2 * cap, hs), bf),
        v((ndp, 2, cap, width), bf),
        v((ndp, 2, cap, width), bf),
        v((nt, 2, cap, width), bf),
        v((nt, 2, cap, width), bf),
        v((nt, 2, cap, width), bf),
    ]
    sems = [
        dma((6,)), dma(()), dma(()), dma(()), dma((ndp,)), dma((ndp,)), dma((ndp,)),
        dma((nt, 2)), dma((nt, 2)), dma((nt, 2)), dma((nt, 2)), dma((nt, 2)),
        dma((2,)), dma((2,)), dma(()), dma(()), dma((ndp,)), dma((ndp,)), dma((ndp,)), dma((ndp,)),
        dma((ndp,)), dma((ndp,)), dma((nt,)), dma((nt,)), dma((nt,)), dma((nt,)),
    ]
    in_vmem = pl.BlockSpec(memory_space=v)
    in_hbm = pl.BlockSpec(memory_space=pl.ANY)
    return pl.pallas_call(
        functools.partial(layer_kernel, (ndp, nt, cap, width)),
        out_shape=jax.ShapeDtypeStruct(tokens.shape, bf),
        in_specs=[in_vmem] * 4 + [in_hbm] * 6,
        out_specs=in_vmem,
        scratch_shapes=scratch + sems,
        compiler_params=pltpu.CompilerParams(
            collective_id=0, has_side_effects=True, vmem_limit_bytes=VMEM_BYTES
        ),
    )(tokens, pick, unpick, router, eg, eu, ed, sg, su, sd)


def fits(mesh):
    return mesh.shape["dp"] == mesh.shape["tensor"] and mesh.shape["dp"] // 2 == 2


def solution(mesh):
    in_specs = (
        P(("group", "dp"), "tensor"),
        P(),
        P(None, ("dp", "tensor")),
        P(None, ("dp", "tensor")),
        P(("dp", "tensor"), None),
        P("dp", "tensor"),
        P("dp", "tensor"),
        P("tensor", "dp"),
        P(("group", "dp")),
        P(("group", "dp")),
    )
    out_specs = P(("group", "dp"), "tensor")
    return jax.shard_map(
        fused if fits(mesh) else on_device, mesh=mesh, in_specs=in_specs, out_specs=out_specs, check_vma=False
    )
```

```python
import functools

import jax
import jax.numpy as jnp
from jax import lax
from jax.experimental import pallas as pl
from jax.experimental.pallas import tpu as pltpu
from jax.sharding import PartitionSpec as P


def on_device(
    tokens,
    router,
    expert_gate,
    expert_up,
    expert_down,
    shared_gate,
    shared_up,
    shared_down,
    expert_ids,
    expert_slots,
):
    tok_rows, part_width = tokens.shape
    dp_count = lax.axis_size("dp")
    experts = dp_count // 2
    capacity = min(2 * tok_rows // experts, tok_rows // 2)
    gathered = lax.all_gather(tokens, "tensor", axis=1, tiled=True)
    logits = jnp.dot(gathered, router, preferred_element_type=jnp.float32)
    one_hot = (expert_ids[:, None] == jnp.arange(experts, dtype=jnp.int32)[None, :]).astype(
        jnp.float32
    )
    gating = jax.nn.sigmoid(jnp.sum(logits * one_hot, axis=1))
    routed = (tokens.astype(jnp.float32) * gating[:, None]).astype(jnp.bfloat16)
    outgoing = (
        jnp.zeros((experts, capacity, part_width), jnp.bfloat16)
        .at[expert_ids, expert_slots]
        .set(routed)
    )
    gate_sum = jnp.dot(
        gathered,
        lax.all_gather(shared_gate, "dp", axis=0, tiled=True),
        preferred_element_type=jnp.float32,
    )
    up_sum = jnp.dot(
        gathered,
        lax.all_gather(shared_up, "dp", axis=0, tiled=True),
        preferred_element_type=jnp.float32,
    )
    shared_hidden = (jax.nn.silu(gate_sum) * up_sum).astype(jnp.bfloat16)
    shared_terms = jnp.dot(
        shared_hidden,
        lax.all_gather(shared_down, "dp", axis=1, tiled=True),
        preferred_element_type=jnp.float32,
    )
    shared_out = lax.psum_scatter(
        shared_terms.astype(jnp.bfloat16), "tensor", scatter_dimension=1, tiled=True
    ).astype(jnp.float32)
    to_send = jnp.repeat(outgoing, 2, axis=0)
    received = lax.all_to_all(to_send, "dp", split_axis=0, concat_axis=0, tiled=True)
    source_count = received.shape[0]
    slot_count = received.shape[1]
    slot_total = source_count * slot_count
    portion = lax.all_gather(received, "tensor", axis=2, tiled=True)
    flattened = portion.reshape(slot_total, portion.shape[2])
    gate_e = jnp.dot(flattened, expert_gate, preferred_element_type=jnp.float32)
    up_e = jnp.dot(flattened, expert_up, preferred_element_type=jnp.float32)
    hidden_e = (jax.nn.silu(gate_e) * up_e).astype(jnp.bfloat16)
    expert_terms = jnp.dot(hidden_e, expert_down, preferred_element_type=jnp.float32)
    expert_terms = expert_terms.reshape(source_count, slot_count, expert_terms.shape[1])
    returned_raw = lax.all_to_all(
        lax.psum_scatter(
            expert_terms.astype(jnp.bfloat16), "tensor", scatter_dimension=2, tiled=True
        ),
        "dp",
        split_axis=0,
        concat_axis=0,
        tiled=True,
    ).astype(jnp.float32)
    returned = (
        returned_raw.reshape(experts, 2, capacity, part_width).sum(axis=1).astype(jnp.bfloat16)
    )
    expert_out = returned[expert_ids, expert_slots]
    return (shared_out + expert_out.astype(jnp.float32)).astype(jnp.bfloat16)


VMEM_BYTES = 64 * 1024 * 1024 - 65536


def tile_of(width):
    return next(t for t in (256, 128, width) if width % t == 0)


def layer_kernel(
    shape,
    tok, pick, unpick, router,
    eg_hbm, eu_hbm, ed_hbm, sg_hbm, su_hbm, sd_hbm,
    out,
    eg, eu, ed, sg, su, sd,
    own, table, rest, logit, acc_g, acc_u, hid_e, part_e, core_e, row_e, pair_e,
    part_s, got_s, hid_s, down_s, gotd_s, left, right, passed,
    wsem, send_y, recv_y, send_q, recv_q, send_ql, send_qr, send_l, send_r, recv_z, send_c, recv_c,
    send_pc, recv_pc, send_py, recv_py, send_gs, recv_gs, send_h, recv_h, send_d, recv_d,
    send_tr, send_tl, recv_tl, recv_tr,
):
    ndp, nt, cap, width = shape
    group, dp, z = (lax.axis_index(n) for n in ("group", "dp", "tensor"))
    y, c = lax.div(dp, 2), lax.rem(dp, 2)
    mate, across = 2 * y + 1 - c, 2 * (1 - y) + c
    others = [lax.rem(dp + i, ndp) for i in range(1, ndp)]
    rows = ndp * cap
    sending = []

    def copy(src, dst, ss, rs, dev_dp, dev_z):
        return pltpu.make_async_remote_copy(
            src_ref=src, dst_ref=dst, send_sem=ss, recv_sem=rs,
            device_id=(group, dev_dp, dev_z), device_id_type=pl.DeviceIdType.MESH,
        )

    def send(cond, make):
        if cond is None:
            make().start()
        else:
            pl.when(cond)(lambda: make().start())
        sending.append((cond, make))

    weights = [
        pltpu.make_async_copy(a, b, wsem.at[i])
        for i, (a, b) in enumerate(
            ((sg_hbm, sg), (su_hbm, su), (eg_hbm, eg), (eu_hbm, eu), (ed_hbm, ed), (sd_hbm, sd))
        )
    ]
    for w in weights:
        w.start()

    barrier = pltpu.get_barrier_semaphore()
    for o in others:
        pl.semaphore_signal(barrier, 1, device_id=(group, o, z), device_id_type=pl.DeviceIdType.MESH)

    @pl.when(z > 0)
    def _():
        pl.semaphore_signal(barrier, 1, device_id=(group, dp, z - 1), device_id_type=pl.DeviceIdType.MESH)

    @pl.when(z < nt - 1)
    def _():
        pl.semaphore_signal(barrier, 1, device_id=(group, dp, z + 1), device_id_type=pl.DeviceIdType.MESH)

    tw = tile_of(width)

    @pl.loop(0, width // tw)
    def _(i):
        cols = pl.ds(pl.multiple_of(i * tw, tw), tw)
        picked = jnp.dot(pick[...], tok[:, cols], preferred_element_type=jnp.float32)
        own[:, :, cols] = picked.astype(jnp.bfloat16).reshape(2, cap, tw)

    table[z, dp] = own[y]

    @pl.when(dp == z)
    def _():
        rest[dp] = own[1 - y]

    at_end = (z == 0) | (z == nt - 1)

    @pl.when(at_end)
    def _():
        pl.semaphore_wait(barrier, ndp)

    @pl.when(jnp.logical_not(at_end))
    def _():
        pl.semaphore_wait(barrier, ndp + 1)

    send(None, lambda: copy(own.at[1 - y], table.at[z, dp], send_y, recv_y, across, z))
    home_row = lax.div(z, 2)
    send(dp != z, lambda: copy(own.at[1 - home_row], rest.at[dp], send_q, recv_q.at[dp], z, z))

    def spread(zs, j, toward_left, toward_right):
        block = table.at[zs, 2 * j + c]
        send(toward_right, lambda: copy(block, block, send_r.at[zs, j], recv_z.at[zs, j], dp, z + 1))
        send(toward_left, lambda: copy(block, block, send_l.at[zs, j], recv_z.at[zs, j], dp, z - 1))

    def to_mate(cond, zs, j):
        block = table.at[zs, 2 * j + c]
        send(cond, lambda: copy(block, block, send_c.at[zs, j], recv_c.at[zs, j], mate, z))

    spread(z, y, z > 0, z < nt - 1)
    to_mate(None, z, y)
    copy(own.at[0], table.at[z, across], send_y, recv_y, across, z).wait_recv()
    spread(z, 1 - y, z > 0, z < nt - 1)
    to_mate(None, z, 1 - y)

    def relay_rest(distance):
        for s in range(ndp):
            for at, go_left, go_right in (
                ((z == dp, z > 0, z < nt - 1),)
                if distance == 0
                else (
                    (z == dp + distance, None, z < nt - 1),
                    (z == dp - distance, z > 0, None),
                )
            ):
                waits = at & (dp != s) if distance == 0 else at

                @pl.when(waits)
                def _():
                    copy(rest.at[s], rest.at[s], send_q, recv_q.at[s], dp, z).wait_recv()

                if go_left is not None:
                    send(at & go_left, lambda s=s: copy(
                        rest.at[s], rest.at[s], send_ql.at[s], recv_q.at[s], dp, z - 1))
                if go_right is not None:
                    send(at & go_right, lambda s=s: copy(
                        rest.at[s], rest.at[s], send_qr.at[s], recv_q.at[s], dp, z + 1))

    te = tile_of(acc_g.shape[1])

    logit[...] = jnp.zeros_like(logit)
    acc_g[...] = jnp.zeros_like(acc_g)
    acc_u[...] = jnp.zeros_like(acc_u)

    def expert_chunk(zs):
        for j in range(2):
            block = table.at[zs, 2 * j + 1 - c]
            copy(block, block, send_c.at[zs, j], recv_c.at[zs, j], mate, z).wait_recv()
        depth = pl.ds(pl.multiple_of(zs * width, width), width)
        x = table.at[zs]
        logit[...] += lax.dot_general(
            x[...].reshape(rows, width), router[:, depth], (((1,), (1,)), ((), ())),
            preferred_element_type=jnp.float32,
        )

        @pl.loop(0, acc_g.shape[1] // te)
        def _(i):
            cols = pl.ds(pl.multiple_of(i * te, te), te)
            xs = x[...].reshape(rows, width)
            acc_g[:, cols] += jnp.dot(xs, eg[depth, cols], preferred_element_type=jnp.float32)
            acc_u[:, cols] += jnp.dot(xs, eu[depth, cols], preferred_element_type=jnp.float32)

    relay_rest(0)
    for distance in range(1, nt):
        for zs, inside, far in (
            (z - distance, z >= distance, "right"),
            (z + distance, z + distance < nt, "left"),
        ):
            for jr in range(2):
                j = y if jr == 0 else 1 - y

                @pl.when(inside)
                def _():
                    block = table.at[zs, 2 * j + c]
                    copy(block, block, send_r.at[zs, j], recv_z.at[zs, j], dp, z).wait_recv()

                block = lambda zs=zs, j=j: table.at[zs, 2 * j + c]
                if far == "right":
                    send(inside & (z < nt - 1), lambda zs=zs, j=j, block=block: copy(
                        block(), block(), send_r.at[zs, j], recv_z.at[zs, j], dp, z + 1))
                else:
                    send(inside & (z > 0), lambda zs=zs, j=j, block=block: copy(
                        block(), block(), send_l.at[zs, j], recv_z.at[zs, j], dp, z - 1))
                send(inside, lambda zs=zs, j=j, block=block: copy(
                    block(), block(), send_c.at[zs, j], recv_c.at[zs, j], mate, z))
        relay_rest(distance)
        if distance == 1:
            for w in weights[:4]:
                w.wait()
            expert_chunk(z)
        else:
            for zs, inside in ((z - distance + 1, z >= distance - 1), (z + distance - 1, z + distance - 1 < nt)):
                pl.when(inside)(functools.partial(expert_chunk, zs))
    last = nt - 1
    for zs, inside in ((z - last, z >= last), (z + last, z + last < nt)):
        pl.when(inside)(functools.partial(expert_chunk, zs))

    hs = sg.shape[1]
    ts = tile_of(hs)

    @pl.loop(0, hs // ts)
    def _(i):
        cols = pl.ds(pl.multiple_of(i * ts, ts), ts)
        for w, k in ((sg, 0), (su, 1)):
            for src, e in ((table.at[dp], y), (rest, 1 - y)):
                part = jnp.dot(
                    src[...].reshape(rows, width), w[:, cols], preferred_element_type=jnp.float32
                )
                part_s[:, e, k, :, cols] = part.astype(jnp.bfloat16).reshape(ndp, cap, ts)

    for e in range(2):
        for i, o in enumerate(others):
            send(None, lambda i=i, o=o, e=e: copy(
                part_s.at[o, e], got_s.at[i, e], send_gs.at[i, e], recv_gs.at[i, e], o, z))

    lanes = lax.broadcasted_iota(jnp.int32, logit.shape, 1)
    gating = jax.nn.sigmoid(jnp.sum(jnp.where(lanes == y, logit[...], 0.0), axis=1, keepdims=True))
    hid_e[...] = (jax.nn.silu(acc_g[...] * gating) * (acc_u[...] * gating)).astype(jnp.bfloat16)
    weights[4].wait()
    per = width // tw

    @pl.loop(0, nt * per)
    def _(i):
        t, n = lax.div(i, per), lax.rem(i, per)
        part = jnp.dot(
            hid_e[...], ed[:, pl.ds(pl.multiple_of(i * tw, tw), tw)],
            preferred_element_type=jnp.float32,
        )
        part_e[:, t, :, pl.ds(pl.multiple_of(n * tw, tw), tw)] = part.astype(
            jnp.bfloat16
        ).reshape(ndp, cap, tw)

    for j in range(2):
        send(None, lambda j=j: copy(
            part_e.at[2 * j + 1 - c], core_e.at[j], send_pc.at[j], recv_pc.at[j], mate, z))

    for e in range(2):
        for i in range(ndp - 1):
            copy(part_s.at[0, e], got_s.at[i, e], send_gs.at[i, e], recv_gs.at[i, e], dp, z).wait_recv()

        @pl.loop(0, hs // ts)
        def _(i, e=e):
            cols = pl.ds(pl.multiple_of(i * ts, ts), ts)
            total = part_s[dp, e, :, :, cols].astype(jnp.float32)
            for k in range(ndp - 1):
                total = total + got_s[k, e, :, :, cols].astype(jnp.float32)
            hid_s[e, dp, :, cols] = (jax.nn.silu(total[0]) * total[1]).astype(jnp.bfloat16)

        for i, o in enumerate(others):
            send(None, lambda i=i, o=o, e=e: copy(
                hid_s.at[e, dp], hid_s.at[e, dp], send_h.at[i, e], recv_h.at[dp, e], o, z))

    for j in range(2):
        copy(part_e.at[0], core_e.at[j], send_pc.at[j], recv_pc.at[j], dp, z).wait_recv()

    @pl.loop(0, nt)
    def _(t):
        both = part_e[across, t].astype(jnp.float32) + core_e[1 - y, t].astype(jnp.float32)
        pair_e[t] = both.astype(jnp.bfloat16)

    send(None, lambda: copy(pair_e, row_e, send_py, recv_py, across, z))

    weights[5].wait()
    for e in range(2):
        for o in others:
            copy(hid_s.at[e, o], hid_s.at[e, o], send_h.at[0, e], recv_h.at[o, e], dp, z).wait_recv()

        @pl.loop(0, width // tw)
        def _(i, e=e):
            cols = pl.ds(pl.multiple_of(i * tw, tw), tw)
            part = jnp.dot(
                hid_s[e].reshape(rows, hs), sd[:, cols], preferred_element_type=jnp.float32
            )
            down_s[:, e, :, cols] = part.astype(jnp.bfloat16).reshape(ndp, cap, tw)

        for i, o in enumerate(others):
            send(None, lambda i=i, o=o, e=e: copy(
                down_s.at[o, e], gotd_s.at[dp, e], send_d.at[i, e], recv_d.at[dp, e], o, z))
        gotd_s[dp, e] = down_s[dp, e]
    copy(pair_e, row_e, send_py, recv_py, dp, z).wait_recv()

    def own_sum(t, e, cols):
        shared = gotd_s[t, e, :, cols].astype(jnp.float32)
        near = part_e[dp, t, :, cols].astype(jnp.float32) + core_e[y, t, :, cols].astype(jnp.float32)
        return shared + jnp.where(e == y, near, row_e[t, :, cols].astype(jnp.float32))

    def combined(t, e, sources):
        @pl.loop(0, per)
        def _(i):
            cols = pl.ds(pl.multiple_of(i * tw, tw), tw)
            total = own_sum(t, e, cols)
            for ref in sources:
                total = total + ref[t, e, :, cols].astype(jnp.float32)
            passed[t, e, :, cols] = total.astype(jnp.bfloat16)

    def arrive(ref, sems, t, e, cond):
        @pl.when(cond)
        def _():
            copy(ref.at[t, e], ref.at[t, e], send_tr.at[t, e], sems.at[t, e], dp, z).wait_recv()

        @pl.when(jnp.logical_not(cond))
        def _():
            ref[t, e] = jnp.zeros(ref.shape[2:], ref.dtype)

    for i in range(nt - 1):
        for e in range(2):
            if i == 0:
                for o in others:
                    copy(gotd_s.at[o, e], gotd_s.at[o, e], send_d.at[0, e], recv_d.at[o, e], dp, z).wait_recv()
            t, u = nt - 1 - i, i

            @pl.when(t > z)
            def _():
                arrive(left, recv_tl, t, e, z > 0)
                combined(t, e, (left,))

            send(t > z, lambda t=t, e=e: copy(
                passed.at[t, e], left.at[t, e], send_tr.at[t, e], recv_tl.at[t, e], dp, z + 1))

            @pl.when(u < z)
            def _():
                arrive(right, recv_tr, u, e, z < nt - 1)
                combined(u, e, (right,))

            send(u < z, lambda u=u, e=e: copy(
                passed.at[u, e], right.at[u, e], send_tl.at[u, e], recv_tr.at[u, e], dp, z - 1))
    for e in range(2):
        arrive(left, recv_tl, z, e, z > 0)
        arrive(right, recv_tr, z, e, z < nt - 1)
        combined(z, e, (left, right))

    @pl.loop(0, per)
    def _(i):
        cols = pl.ds(pl.multiple_of(i * tw, tw), tw)
        slots = passed[z, :, :, cols].reshape(2 * cap, tw)
        out[:, cols] = jnp.dot(unpick[...], slots, preferred_element_type=jnp.float32).astype(
            jnp.bfloat16
        )

    for cond, make in sending:
        if cond is None:
            make().wait_send()
        else:
            pl.when(cond)(lambda make=make: make().wait_send())


def fused(tokens, router, eg, eu, ed, sg, su, sd, ids, slots):
    ndp, nt = lax.axis_size("dp"), lax.axis_size("tensor")
    tok_rows, width = tokens.shape
    cap = min(2 * tok_rows // 2, tok_rows // 2)
    spot = ids * cap + slots
    pick = (jnp.arange(2 * cap, dtype=jnp.int32)[:, None] == spot[None, :]).astype(jnp.bfloat16)
    unpick = (spot[:, None] == jnp.arange(2 * cap, dtype=jnp.int32)[None, :]).astype(jnp.bfloat16)
    bf, f32 = jnp.bfloat16, jnp.float32
    rows, hid, hs, depth = ndp * cap, eg.shape[1], sg.shape[1], eg.shape[0]
    v = pltpu.VMEM
    dma = pltpu.SemaphoreType.DMA
    scratch = [v(w.shape, bf) for w in (eg, eu, ed, sg, su, sd)] + [
        v((2, cap, width), bf),
        v((nt, ndp, cap, width), bf),
        v((ndp, cap, width), bf),
        v((rows, router.shape[1]), f32),
        v((rows, hid), f32),
        v((rows, hid), f32),
        v((rows, hid), bf),
        v((ndp, nt, cap, width), bf),
        v((2, nt, cap, width), bf),
        v((nt, cap, width), bf),
        v((nt, cap, width), bf),
        v((ndp, 2, 2, cap, hs), bf),
        v((ndp - 1, 2, 2, cap, hs), bf),
        v((2, ndp, cap, hs), bf),
        v((ndp, 2, cap, width), bf),
        v((ndp, 2, cap, width), bf),
        v((nt, 2, cap, width), bf),
        v((nt, 2, cap, width), bf),
        v((nt, 2, cap, width), bf),
    ]
    sems = [
        dma((6,)), dma(()), dma(()), dma(()), dma((ndp,)), dma((ndp,)), dma((ndp,)),
        dma((nt, 2)), dma((nt, 2)), dma((nt, 2)), dma((nt, 2)), dma((nt, 2)),
        dma((2,)), dma((2,)), dma(()), dma(()),
        *[dma((ndp, 2))] * 6, *[dma((nt, 2))] * 4,
    ]
    in_vmem = pl.BlockSpec(memory_space=v)
    in_hbm = pl.BlockSpec(memory_space=pl.ANY)
    return pl.pallas_call(
        functools.partial(layer_kernel, (ndp, nt, cap, width)),
        out_shape=jax.ShapeDtypeStruct(tokens.shape, bf),
        in_specs=[in_vmem] * 4 + [in_hbm] * 6,
        out_specs=in_vmem,
        scratch_shapes=scratch + sems,
        compiler_params=pltpu.CompilerParams(
            collective_id=0, has_side_effects=True, vmem_limit_bytes=VMEM_BYTES
        ),
    )(tokens, pick, unpick, router.T, eg, eu, ed, sg, su, sd)


def fits(mesh):
    return mesh.shape["dp"] == mesh.shape["tensor"] and mesh.shape["dp"] // 2 == 2


def solution(mesh):
    in_specs = (
        P(("group", "dp"), "tensor"),
        P(),
        P(None, ("dp", "tensor")),
        P(None, ("dp", "tensor")),
        P(("dp", "tensor"), None),
        P("dp", "tensor"),
        P("dp", "tensor"),
        P("tensor", "dp"),
        P(("group", "dp")),
        P(("group", "dp")),
    )
    out_specs = P(("group", "dp"), "tensor")
    return jax.shard_map(
        fused if fits(mesh) else on_device, mesh=mesh, in_specs=in_specs, out_specs=out_specs, check_vma=False
    )
```
